8 devices in a mesh: model: 2 (over z, y), sub: 2 (over x), data: 2 (over core).
Axes of the slice: x: 2, y: 2, z: 1, core: 2. Of those that a mesh axis runs over, the one named last changes fastest.
Arguments:
- images: bfloat16 [24, 576, 768], P(('model', 'sub', 'data'))
- targets: bfloat16 [24, 576, 768], P(('model', 'sub', 'data'))
- w_in: float32 [6, 768, 3072], replicated
- w_out: float32 [6, 3072, 768], replicated
Outputs:
- output 1: float32 [6, 768, 3072], replicated
- output 2: float32 [6, 3072, 768], replicated
- output 3: float32 [], replicated
All inputs are finite; a program needn't handle non-finite values.
Results may differ from the reference program's by a relative error of at most 0.00469329.
Values are sent between devices in bfloat16 or wider.
A program may use at most 1 GiB of HBM per device.

```python
import jax
import jax.numpy as jnp
import math
from jax import lax

D = 768
FF = 3072
SEQ = 576
LAYERS = 6
IMGS_DEV = 3
DEVICES = 8
IMAGES = IMGS_DEV * DEVICES
TOKENS = IMAGES * SEQ
BLOCK_ROWS = IMGS_DEV * SEQ
INV_COUNT = 1.0 / (TOKENS * D)
RHO_REL = 0.1
RADIUS = RHO_REL * math.sqrt(LAYERS * FF + D)
LEARN_RATE = 8.0
SQRT_HALF = 0.7071067811865476
INV_SQRT_2PI = 0.3989422804014327


def setup_inputs(seed: int = 0) -> dict:
    root_key = jax.random.key(seed)
    subkeys = jax.random.split(root_key, 8)
    img_shift = 0.8 * jax.random.normal(subkeys[0], (IMAGES, 1, D), jnp.float32)
    img_gain = jnp.exp(0.3 * jax.random.normal(subkeys[1], (IMAGES, 1, 1), jnp.float32))
    images = jax.random.normal(subkeys[2], (IMAGES, SEQ, D), jnp.float32) * img_gain + img_shift
    tgt_shift = 0.5 * jax.random.normal(subkeys[3], (1, 1, D), jnp.float32) + 0.8 * jax.random.normal(subkeys[4], (IMAGES, 1, D), jnp.float32)
    targets = jax.random.normal(subkeys[5], (IMAGES, SEQ, D), jnp.float32) + tgt_shift
    w_in = jax.random.normal(subkeys[6], (LAYERS, D, FF), jnp.float32) * D ** -0.5
    w_out = jax.random.normal(subkeys[7], (LAYERS, FF, D), jnp.float32) * (FF * LAYERS) ** -0.5
    return {'images': images.astype(jnp.bfloat16), 'targets': targets.astype(jnp.bfloat16), 'w_in': w_in, 'w_out': w_out}


def gelu_fn(pre_act):
    return 0.5 * pre_act * (1.0 + lax.erf(pre_act * SQRT_HALF))


def gelu_slope(pre_act):
    cdf_part = 0.5 * (1.0 + lax.erf(pre_act * SQRT_HALF))
    return cdf_part + pre_act * INV_SQRT_2PI * jnp.exp(-0.5 * pre_act * pre_act)


def layer_forward(hidden, weights):
    w_in_l, w_out_l = weights
    pre_act = jnp.dot(hidden, w_in_l, preferred_element_type=jnp.float32).astype(jnp.bfloat16)
    post_act = gelu_fn(pre_act.astype(jnp.float32)).astype(jnp.bfloat16)
    mlp_out = jnp.dot(post_act, w_out_l, preferred_element_type=jnp.float32)
    new_hidden = (hidden.astype(jnp.float32) + mlp_out).astype(jnp.bfloat16)
    return new_hidden, (hidden, pre_act, post_act)


def layer_backward(d_hidden, inputs_l):
    hidden, pre_act, post_act, w_in_l, w_out_l = inputs_l
    grad_out = jnp.dot(post_act.T, d_hidden, preferred_element_type=jnp.float32)
    d_act = jnp.dot(d_hidden, w_out_l.T, preferred_element_type=jnp.float32)
    d_pre = (d_act * gelu_slope(pre_act.astype(jnp.float32))).astype(jnp.bfloat16)
    grad_in = jnp.dot(hidden.T, d_pre, preferred_element_type=jnp.float32)
    d_prev = (d_hidden.astype(jnp.float32) + jnp.dot(d_pre, w_in_l.T, preferred_element_type=jnp.float32)).astype(jnp.bfloat16)
    return d_prev, (grad_in, grad_out)


def block_grads(x_rows, y_rows, w_in_bf, w_out_bf):
    top_hidden, saved_acts = lax.scan(layer_forward, x_rows, (w_in_bf, w_out_bf))
    resid_err = top_hidden.astype(jnp.float32) - y_rows.astype(jnp.float32)
    d_top = (resid_err * INV_COUNT).astype(jnp.bfloat16)
    hiddens, pre_acts, post_acts = saved_acts
    _, grads = lax.scan(layer_backward, d_top, (hiddens, pre_acts, post_acts, w_in_bf, w_out_bf), reverse=True)
    return 0.5 * jnp.sum(resid_err * resid_err), grads[0], grads[1]


def full_grads(images, targets, w_in_bf, w_out_bf):
    x_blocks = images.reshape(DEVICES, BLOCK_ROWS, D)
    y_blocks = targets.reshape(DEVICES, BLOCK_ROWS, D)

    def accumulate(totals, block_pair):
        loss_blk, gin_blk, gout_blk = block_grads(block_pair[0], block_pair[1], w_in_bf, w_out_bf)
        return (totals[0] + loss_blk, totals[1] + gin_blk, totals[2] + gout_blk), None

    init_carry = (jnp.zeros((), jnp.float32), jnp.zeros((LAYERS, D, FF), jnp.float32), jnp.zeros((LAYERS, FF, D), jnp.float32))
    totals, _ = lax.scan(accumulate, init_carry, (x_blocks, y_blocks))
    return totals


def reference(images, targets, w_in, w_out):
    _, grad_in, grad_out = full_grads(images, targets, w_in.astype(jnp.bfloat16), w_out.astype(jnp.bfloat16))
    grad_norm = jnp.sqrt(jnp.sum(grad_in * grad_in) + jnp.sum(grad_out * grad_out))
    step_scale = RADIUS / grad_norm
    pert_in = (w_in + step_scale * grad_in).astype(jnp.bfloat16)
    pert_out = (w_out + step_scale * grad_out).astype(jnp.bfloat16)
    loss_sum, grad2_in, grad2_out = full_grads(images, targets, pert_in, pert_out)
    return (w_in - LEARN_RATE * grad2_in, w_out - LEARN_RATE * grad2_out, loss_sum * INV_COUNT)
```

```python
import jax
import jax.numpy as jnp
import math
from jax import lax
from jax.experimental.layout import Layout, with_layout_constraint
from jax.sharding import PartitionSpec as P

RHO_REL = 0.1
LEARN_RATE = 8.0
SQRT_HALF = 0.7071067811865476
INV_SQRT_2PI = 0.3989422804014327


def gelu_fn(pre_act):
    return 0.5 * pre_act * (1.0 + lax.erf(pre_act * SQRT_HALF))


def gelu_slope(pre_act):
    cdf_part = 0.5 * (1.0 + lax.erf(pre_act * SQRT_HALF))
    return cdf_part + pre_act * INV_SQRT_2PI * jnp.exp(-0.5 * pre_act * pre_act)


def forward(x_rows, in_list, out_list):
    hidden = x_rows
    saved_acts = []
    for layer_idx in range(len(in_list)):
        pre_act = jnp.dot(hidden, in_list[layer_idx], preferred_element_type=jnp.float32).astype(jnp.bfloat16)
        post_act = gelu_fn(pre_act.astype(jnp.float32)).astype(jnp.bfloat16)
        mlp_out = jnp.dot(post_act, out_list[layer_idx], preferred_element_type=jnp.float32)
        saved_acts.append((hidden, pre_act, post_act))
        hidden = (hidden.astype(jnp.float32) + mlp_out).astype(jnp.bfloat16)
    return hidden, saved_acts


def backward(d_top, saved_acts, in_list, out_list, reduce_fn, finish_fn, ahead=3):
    d_hidden = d_top
    n_layers = len(saved_acts)
    pending, finished = [], {}

    def due(value, count):
        while len(pending) > count:
            unit, shard = pending.pop(0)
            finished[unit], value = lax.optimization_barrier((finish_fn(unit, shard), value))
        return value

    for layer_idx in reversed(range(n_layers)):
        hidden, pre_act, post_act = saved_acts[layer_idx]
        d_hidden = due(d_hidden, ahead - 1)
        grad_out = row_major(jnp.einsum('tf,td->fd', post_act, d_hidden, preferred_element_type=jnp.float32))
        grad_out, d_hidden = lax.optimization_barrier((grad_out, d_hidden))
        pending.append((('out', layer_idx), reduce_fn(grad_out)))
        d_hidden = due(d_hidden, ahead - 1)
        d_act = jnp.einsum('td,fd->tf', d_hidden, out_list[layer_idx], preferred_element_type=jnp.float32)
        d_pre = (d_act * gelu_slope(pre_act.astype(jnp.float32))).astype(jnp.bfloat16)
        grad_in = row_major(jnp.einsum('td,tf->df', hidden, d_pre, preferred_element_type=jnp.float32))
        grad_in, d_pre = lax.optimization_barrier((grad_in, d_pre))
        pending.append((('in', layer_idx), reduce_fn(grad_in)))
        if layer_idx > 0:
            back_part = jnp.einsum('tf,df->td', d_pre, in_list[layer_idx], preferred_element_type=jnp.float32)
            d_hidden = (d_hidden.astype(jnp.float32) + back_part).astype(jnp.bfloat16)
    for unit, shard in pending:
        finished[unit] = finish_fn(unit, shard)
    return finished


def row_major(matrix):
    return with_layout_constraint(matrix, Layout(major_to_minor=(0, 1)))


def top_grad(top_hidden, y_rows, inv_count):
    resid_err = top_hidden.astype(jnp.float32) - y_rows.astype(jnp.float32)
    return 0.5 * jnp.sum(resid_err * resid_err), (resid_err * inv_count).astype(jnp.bfloat16)


def solution(mesh):
    mesh_axes = tuple(mesh.axis_names)
    dev_count = math.prod([mesh.shape[axis_name] for axis_name in mesh_axes])
    batch_spec = P(mesh_axes, None, None)

    def local_step(images, targets, w_in, w_out):
        layers, model_dim, hidden_dim = w_in.shape
        tok_local = images.shape[0] * images.shape[1]
        inv_count = 1.0 / (tok_local * dev_count * model_dim)
        radius = RHO_REL * math.sqrt(layers * hidden_dim + model_dim)
        x_rows = images.reshape(tok_local, model_dim)
        y_rows = targets.reshape(tok_local, model_dim)
        my_index = lax.axis_index(mesh_axes)
        rows_in = model_dim // dev_count
        rows_out = hidden_dim // dev_count

        def scatter(grad):
            return row_major(lax.psum_scatter(grad, mesh_axes, scatter_dimension=0, tiled=True))

        def gather(shard):
            return lax.all_gather(shard, mesh_axes, axis=0, tiled=True)

        in_list = [w_in[layer_idx].astype(jnp.bfloat16) for layer_idx in range(layers)]
        out_list = [w_out[layer_idx].astype(jnp.bfloat16) for layer_idx in range(layers)]
        top_hidden, saved_acts = forward(x_rows, in_list, out_list)
        _, d_top = top_grad(top_hidden, y_rows, inv_count)
        w_mine = {}
        for layer_idx in range(layers):
            w_mine['in', layer_idx] = lax.dynamic_slice(w_in, (layer_idx, my_index * rows_in, 0), (1, rows_in, hidden_dim))[0]
            w_mine['out', layer_idx] = lax.dynamic_slice(w_out, (layer_idx, my_index * rows_out, 0), (1, rows_out, model_dim))[0]

        first = backward(d_top, saved_acts, in_list, out_list, scatter, lambda unit, shard: (shard, jnp.sum(shard * shard)))
        norm_sq = lax.psum(sum(part_sq for _, part_sq in first.values()), mesh_axes)
        step_scale = radius / jnp.sqrt(norm_sq)

        def perturbed(unit):
            return gather((w_mine[unit] + step_scale * first[unit][0]).astype(jnp.bfloat16))

        pert_in, pert_out = [], []
        for layer_idx in range(layers):
            pert_in.append(perturbed(('in', layer_idx)))
            pert_out.append(perturbed(('out', layer_idx)))

        top_pert, saved_pert = forward(x_rows, pert_in, pert_out)
        loss_local, d_pert = top_grad(top_pert, y_rows, inv_count)
        second = backward(d_pert, saved_pert, pert_in, pert_out, scatter, lambda unit, shard: shard)
        loss_total = lax.psum(loss_local, mesh_axes)
        full = {unit: gather(shard) for unit, shard in second.items()}
        new_in = [w_in[layer_idx] - LEARN_RATE * full['in', layer_idx] for layer_idx in range(layers)]
        new_out = [w_out[layer_idx] - LEARN_RATE * full['out', layer_idx] for layer_idx in range(layers)]
        return jnp.stack(new_in), jnp.stack(new_out), loss_total * inv_count

    return jax.shard_map(local_step, mesh=mesh, in_specs=(batch_spec, batch_spec, P(), P()), out_specs=(P(), P(), P()), check_vma=False)
```

```python
import jax
import jax.numpy as jnp
import math
from jax import lax
from jax.experimental.layout import Layout, with_layout_constraint
from jax.sharding import PartitionSpec as P

RHO_REL = 0.1
LEARN_RATE = 8.0
SQRT_HALF = 0.7071067811865476
INV_SQRT_2PI = 0.3989422804014327


def gelu_fn(pre_act):
    return 0.5 * pre_act * (1.0 + lax.erf(pre_act * SQRT_HALF))


def gelu_slope(pre_act):
    cdf_part = 0.5 * (1.0 + lax.erf(pre_act * SQRT_HALF))
    return cdf_part + pre_act * INV_SQRT_2PI * jnp.exp(-0.5 * pre_act * pre_act)


def forward(x_rows, in_list, out_list):
    hidden = x_rows
    saved_acts = []
    for layer_idx in range(len(in_list)):
        pre_act = jnp.dot(hidden, in_list[layer_idx], preferred_element_type=jnp.float32).astype(jnp.bfloat16)
        post_act = gelu_fn(pre_act.astype(jnp.float32)).astype(jnp.bfloat16)
        mlp_out = jnp.dot(post_act, out_list[layer_idx], preferred_element_type=jnp.float32)
        saved_acts.append((hidden, pre_act, post_act))
        hidden = (hidden.astype(jnp.float32) + mlp_out).astype(jnp.bfloat16)
    return hidden, saved_acts


def backward(d_top, saved_acts, in_list, out_list, reduce_fn, finish_fn, groups):
    d_hidden = d_top
    n_layers = len(saved_acts)
    made, waiting, finished = {}, [], {}

    def due(value, unit_idx):
        while waiting and waiting[0][0] <= unit_idx:
            _, kind, members, shard = waiting.pop(0)
            shard, value = lax.optimization_barrier((finish_fn(kind, members, shard), value))
            finished[kind, members] = shard
        return value

    def launch(kind, layer_idx, grad):
        made[kind, layer_idx] = grad
        for group_kind, members, due_unit in groups:
            if group_kind == kind and min(members) == layer_idx:
                parts = [made[kind, member] for member in members]
                joined = parts[0] if len(parts) == 1 else row_major(jnp.concatenate(parts, axis=1))
                waiting.append((due_unit, kind, members, reduce_fn(joined)))

    for layer_idx in reversed(range(n_layers)):
        unit_idx = 2 * (n_layers - 1 - layer_idx)
        hidden, pre_act, post_act = saved_acts[layer_idx]
        d_hidden = due(d_hidden, unit_idx)
        grad_out = row_major(jnp.einsum('tf,td->fd', post_act, d_hidden, preferred_element_type=jnp.float32))
        grad_out, d_hidden = lax.optimization_barrier((grad_out, d_hidden))
        launch('out', layer_idx, grad_out)
        d_hidden = due(d_hidden, unit_idx + 1)
        d_act = jnp.einsum('td,fd->tf', d_hidden, out_list[layer_idx], preferred_element_type=jnp.float32)
        d_pre = (d_act * gelu_slope(pre_act.astype(jnp.float32))).astype(jnp.bfloat16)
        grad_in = row_major(jnp.einsum('td,tf->df', hidden, d_pre, preferred_element_type=jnp.float32))
        grad_in, d_pre = lax.optimization_barrier((grad_in, d_pre))
        launch('in', layer_idx, grad_in)
        if layer_idx > 0:
            back_part = jnp.einsum('tf,df->td', d_pre, in_list[layer_idx], preferred_element_type=jnp.float32)
            d_hidden = (d_hidden.astype(jnp.float32) + back_part).astype(jnp.bfloat16)
    for _, kind, members, shard in waiting:
        finished[kind, members] = finish_fn(kind, members, shard)
    return finished


def reduce_groups(n_layers):
    last, groups = 2 * n_layers, []
    for top, size, due_out in ((n_layers - 1, 1, 4), (n_layers - 2, 2, 8), (n_layers - 4, n_layers - 3, last)):
        members = tuple(range(top, top - size, -1))
        groups += [('out', members, due_out), ('in', members, due_out + (3 if size == 2 else 1))]
    return groups


def per_layer(groups_done, width):
    split = {}
    for (kind, members), shard in groups_done.items():
        for pos, layer_idx in enumerate(members):
            split[kind, layer_idx] = lax.slice_in_dim(shard, pos * width[kind], (pos + 1) * width[kind], axis=1)
    return split


def row_major(matrix):
    return with_layout_constraint(matrix, Layout(major_to_minor=(0, 1)))


def top_grad(top_hidden, y_rows, inv_count):
    resid_err = top_hidden.astype(jnp.float32) - y_rows.astype(jnp.float32)
    return 0.5 * jnp.sum(resid_err * resid_err), (resid_err * inv_count).astype(jnp.bfloat16)


def solution(mesh):
    mesh_axes = tuple(mesh.axis_names)
    dev_count = math.prod([mesh.shape[axis_name] for axis_name in mesh_axes])
    batch_spec = P(mesh_axes, None, None)

    def local_step(images, targets, w_in, w_out):
        layers, model_dim, hidden_dim = w_in.shape
        tok_local = images.shape[0] * images.shape[1]
        inv_count = 1.0 / (tok_local * dev_count * model_dim)
        radius = RHO_REL * math.sqrt(layers * hidden_dim + model_dim)
        x_rows = images.reshape(tok_local, model_dim)
        y_rows = targets.reshape(tok_local, model_dim)
        my_index = lax.axis_index(mesh_axes)
        rows_in = model_dim // dev_count
        rows_out = hidden_dim // dev_count

        def scatter(grad):
            return row_major(lax.psum_scatter(grad, mesh_axes, scatter_dimension=0, tiled=True))

        def gather(shard):
            return lax.all_gather(shard, mesh_axes, axis=0, tiled=True)

        in_list = [w_in[layer_idx].astype(jnp.bfloat16) for layer_idx in range(layers)]
        out_list = [w_out[layer_idx].astype(jnp.bfloat16) for layer_idx in range(layers)]
        top_hidden, saved_acts = forward(x_rows, in_list, out_list)
        _, d_top = top_grad(top_hidden, y_rows, inv_count)
        width = {'in': hidden_dim, 'out': model_dim}
        groups = reduce_groups(layers)

        def mine(kind, layer_idx):
            if kind == 'in':
                return lax.dynamic_slice(w_in, (layer_idx, my_index * rows_in, 0), (1, rows_in, hidden_dim))[0]
            return lax.dynamic_slice(w_out, (layer_idx, my_index * rows_out, 0), (1, rows_out, model_dim))[0]

        def gather_layers(kind, members, shards):
            joined = shards[0] if len(shards) == 1 else row_major(jnp.concatenate(shards, axis=1))
            return per_layer({(kind, members): gather(joined)}, width)

        first = backward(d_top, saved_acts, in_list, out_list, scatter, lambda kind, members, shard: (shard, jnp.sum(shard * shard)), groups)
        norm_sq = lax.psum(sum(part_sq for _, part_sq in first.values()), mesh_axes)
        step_scale = radius / jnp.sqrt(norm_sq)
        first = per_layer({group: shard for group, (shard, _) in first.items()}, width)
        pert = {}
        for members in ((0,), (1, 2), (3, 4), (5,)):
            for kind in ('in', 'out'):
                shards = [(mine(kind, layer_idx) + step_scale * first[kind, layer_idx]).astype(jnp.bfloat16) for layer_idx in members]
                pert.update(gather_layers(kind, members, shards))
        pert_in = [pert['in', layer_idx] for layer_idx in range(layers)]
        pert_out = [pert['out', layer_idx] for layer_idx in range(layers)]

        top_pert, saved_pert = forward(x_rows, pert_in, pert_out)
        loss_local, d_pert = top_grad(top_pert, y_rows, inv_count)
        second = per_layer(backward(d_pert, saved_pert, pert_in, pert_out, scatter, lambda kind, members, shard: shard, groups), width)
        loss_total = lax.psum(loss_local, mesh_axes)
        full = {}
        for members in ((5, 4, 3), (2, 1, 0)):
            for kind in ('out', 'in'):
                full.update(gather_layers(kind, members, [second[kind, layer_idx] for layer_idx in members]))
        new_in = [w_in[layer_idx] - LEARN_RATE * full['in', layer_idx] for layer_idx in range(layers)]
        new_out = [w_out[layer_idx] - LEARN_RATE * full['out', layer_idx] for layer_idx in range(layers)]
        return jnp.stack(new_in), jnp.stack(new_out), loss_total * inv_count

    return jax.shard_map(local_step, mesh=mesh, in_specs=(batch_spec, batch_spec, P(), P()), out_specs=(P(), P(), P()), check_vma=False)
```

```python
import jax
import jax.numpy as jnp
import math
from jax import lax
from jax.experimental.layout import Layout, with_layout_constraint
from jax.sharding import PartitionSpec as P

RHO_REL = 0.1
LEARN_RATE = 8.0
SQRT_HALF = 0.7071067811865476
INV_SQRT_2PI = 0.3989422804014327


def gelu_fn(pre_act):
    return 0.5 * pre_act * (1.0 + lax.erf(pre_act * SQRT_HALF))


def gelu_slope(pre_act):
    cdf_part = 0.5 * (1.0 + lax.erf(pre_act * SQRT_HALF))
    return cdf_part + pre_act * INV_SQRT_2PI * jnp.exp(-0.5 * pre_act * pre_act)


def forward(x_rows, in_list, out_list):
    hidden = x_rows
    saved_acts = []
    for layer_idx in range(len(in_list)):
        pre_act = jnp.dot(hidden, in_list[layer_idx], preferred_element_type=jnp.float32).astype(jnp.bfloat16)
        post_act = gelu_fn(pre_act.astype(jnp.float32)).astype(jnp.bfloat16)
        mlp_out = jnp.dot(post_act, out_list[layer_idx], preferred_element_type=jnp.float32)
        saved_acts.append((hidden, pre_act, post_act))
        hidden = (hidden.astype(jnp.float32) + mlp_out).astype(jnp.bfloat16)
    return hidden, saved_acts


def backward(d_top, saved_acts, in_list, out_list, reduce_fn, finish_fn, groups):
    d_hidden = d_top
    n_layers = len(saved_acts)
    made, waiting, finished = {}, [], {}

    def due(value, unit_idx):
        while waiting and waiting[0][0] <= unit_idx:
            _, kind, members, shard = waiting.pop(0)
            shard, value = lax.optimization_barrier((finish_fn(kind, members, shard), value))
            finished[kind, members] = shard
        return value

    def launch(kind, layer_idx, grad):
        made[kind, layer_idx] = grad
        for group_kind, members, due_unit in groups:
            if group_kind == kind and min(members) == layer_idx:
                parts = [made[kind, member] for member in members]
                joined = parts[0] if len(parts) == 1 else row_major(jnp.concatenate(parts, axis=1))
                waiting.append((due_unit, kind, members, reduce_fn(joined)))

    for layer_idx in reversed(range(n_layers)):
        unit_idx = 2 * (n_layers - 1 - layer_idx)
        hidden, pre_act, post_act = saved_acts[layer_idx]
        d_hidden = due(d_hidden, unit_idx)
        grad_out = row_major(jnp.einsum('tf,td->fd', post_act, d_hidden, preferred_element_type=jnp.float32))
        grad_out, d_hidden = lax.optimization_barrier((grad_out, d_hidden))
        launch('out', layer_idx, grad_out)
        d_hidden = due(d_hidden, unit_idx + 1)
        d_act = jnp.einsum('td,fd->tf', d_hidden, out_list[layer_idx], preferred_element_type=jnp.float32)
        d_pre = (d_act * gelu_slope(pre_act.astype(jnp.float32))).astype(jnp.bfloat16)
        grad_in = row_major(jnp.einsum('td,tf->df', hidden, d_pre, preferred_element_type=jnp.float32))
        grad_in, d_pre = lax.optimization_barrier((grad_in, d_pre))
        launch('in', layer_idx, grad_in)
        if layer_idx > 0:
            back_part = jnp.einsum('tf,df->td', d_pre, in_list[layer_idx], preferred_element_type=jnp.float32)
            d_hidden = (d_hidden.astype(jnp.float32) + back_part).astype(jnp.bfloat16)
    for _, kind, members, shard in waiting:
        finished[kind, members] = finish_fn(kind, members, shard)
    return finished


def reduce_groups(n_layers):
    last, groups = 2 * n_layers, []
    for top, size, due_out in ((n_layers - 1, 1, 4), (n_layers - 2, 2, 8), (n_layers - 4, n_layers - 3, last)):
        members = tuple(range(top, top - size, -1))
        groups += [('out', members, due_out), ('in', members, due_out + (3 if size == 2 else 1))]
    return groups


def per_layer(groups_done, width):
    split = {}
    for (kind, members), shard in groups_done.items():
        for pos, layer_idx in enumerate(members):
            split[kind, layer_idx] = lax.slice_in_dim(shard, pos * width[kind], (pos + 1) * width[kind], axis=1)
    return split


def row_major(matrix):
    return with_layout_constraint(matrix, Layout(major_to_minor=(0, 1)))


def top_grad(top_hidden, y_rows, inv_count):
    resid_err = top_hidden.astype(jnp.float32) - y_rows.astype(jnp.float32)
    return 0.5 * jnp.sum(resid_err * resid_err), (resid_err * inv_count).astype(jnp.bfloat16)


def solution(mesh):
    mesh_axes = tuple(mesh.axis_names)
    dev_count = math.prod([mesh.shape[axis_name] for axis_name in mesh_axes])
    batch_spec = P(mesh_axes, None, None)

    def local_step(images, targets, w_in, w_out):
        layers, model_dim, hidden_dim = w_in.shape
        tok_local = images.shape[0] * images.shape[1]
        inv_count = 1.0 / (tok_local * dev_count * model_dim)
        radius = RHO_REL * math.sqrt(layers * hidden_dim + model_dim)
        x_rows = images.reshape(tok_local, model_dim)
        y_rows = targets.reshape(tok_local, model_dim)
        my_index = lax.axis_index(mesh_axes)
        rows_in = model_dim // dev_count
        rows_out = hidden_dim // dev_count

        def scatter(grad):
            return row_major(lax.psum_scatter(grad, mesh_axes, scatter_dimension=0, tiled=True))

        def gather(shard):
            return lax.all_gather(shard, mesh_axes, axis=0, tiled=True)

        in_list = [w_in[layer_idx].astype(jnp.bfloat16) for layer_idx in range(layers)]
        out_list = [w_out[layer_idx].astype(jnp.bfloat16) for layer_idx in range(layers)]
        top_hidden, saved_acts = forward(x_rows, in_list, out_list)
        _, d_top = top_grad(top_hidden, y_rows, inv_count)
        width = {'in': hidden_dim, 'out': model_dim}
        groups = reduce_groups(layers)

        def mine(kind, layer_idx):
            if kind == 'in':
                return lax.dynamic_slice(w_in, (layer_idx, my_index * rows_in, 0), (1, rows_in, hidden_dim))[0]
            return lax.dynamic_slice(w_out, (layer_idx, my_index * rows_out, 0), (1, rows_out, model_dim))[0]

        def gather_layers(kind, members, shards):
            joined = shards[0] if len(shards) == 1 else row_major(jnp.concatenate(shards, axis=1))
            return per_layer({(kind, members): gather(joined)}, width)

        first = backward(d_top, saved_acts, in_list, out_list, scatter, lambda kind, members, shard: (shard, jnp.sum(shard * shard)), groups)
        norm_sq = lax.psum(sum(part_sq for _, part_sq in first.values()), mesh_axes)
        step_scale = radius / jnp.sqrt(norm_sq)
        first = per_layer({group: shard for group, (shard, _) in first.items()}, width)
        pert = {}
        for members in ((0,), (1, 2), (3, 4), (5,)):
            for kind in ('in', 'out'):
                shards = [(mine(kind, layer_idx) + step_scale * first[kind, layer_idx]).astype(jnp.bfloat16) for layer_idx in members]
                pert.update(gather_layers(kind, members, shards))
        pert_in = [pert['in', layer_idx] for layer_idx in range(layers)]
        pert_out = [pert['out', layer_idx] for layer_idx in range(layers)]

        top_pert, saved_pert = forward(x_rows, pert_in, pert_out)
        loss_local, d_pert = top_grad(top_pert, y_rows, inv_count)
        second = per_layer(backward(d_pert, saved_pert, pert_in, pert_out, scatter, lambda kind, members, shard: shard, groups), width)
        loss_total = lax.psum(loss_local, mesh_axes)
        full = {}
        down = tuple(reversed(range(layers)))
        all_out = gather(row_major(jnp.concatenate([second['out', layer_idx] for layer_idx in down], axis=1)))
        most_in = gather(row_major(jnp.concatenate([second['in', layer_idx] for layer_idx in down[:-1]], axis=1)))
        all_out, most_in, last_in = lax.optimization_barrier((all_out, most_in, second['in', 0]))
        full.update(per_layer({('out', down): all_out, ('in', down[:-1]): most_in}, width))
        full.update(gather_layers('in', (0,), [last_in]))
        new_in = [w_in[layer_idx] - LEARN_RATE * full['in', layer_idx] for layer_idx in range(layers)]
        new_out = [w_out[layer_idx] - LEARN_RATE * full['out', layer_idx] for layer_idx in range(layers)]
        return jnp.stack(new_in), jnp.stack(new_out), loss_total * inv_count

    return jax.shard_map(local_step, mesh=mesh, in_specs=(batch_spec, batch_spec, P(), P()), out_specs=(P(), P(), P()), check_vma=False)
```
